256 devices in a mesh: row: 16 (over z, core), col: 16 (over y, x).
Axes of the slice: x: 4, y: 4, z: 8, core: 2. Of those that a mesh axis runs over, the one named last changes fastest.
Arguments:
- blocks: bfloat16 [256, 32, 256, 256], P('row', 'col'), may hold values from -0.0625 to 0.0625
- block_cols: int32 [256, 32], P('row', 'col'), may hold values from 0 to 48, as said below
- objective: float32 [196608], P(('col', 'row')), may hold values from -6 to 6
- lower_bound: float32 [196608], P(('col', 'row')), may hold values from -1 to -0.2
- upper_bound: float32 [196608], P(('col', 'row')), may hold values from 0.2 to 1
- right_side: float32 [65536], P(('row', 'col')), may hold values from -6 to 6
- primal_init: float32 [196608], P(('col', 'row')), may hold values from -0.2 to 0.2
- dual_init: float32 [65536], P(('row', 'col')), may hold values from 0 to 1
Outputs:
- primal_final: float32 [196608], P(('col', 'row'))
- dual_final: float32 [65536], P(('row', 'col'))
- step_norms: float32 [8, 2], replicated
The draws below stay inside these ranges and needn't reach their ends.
Inputs may be any that keep to these rules, and one draw needn't show every extreme that they name: `block_cols`: entry j of a row block indexes column group j // 2; its live entries (below 48) are distinct within one row block and group, 48 marks an empty slot, and in every draw some row block has all 2 slots of some group live.
All inputs are finite; a program needn't handle non-finite values.
Results may differ from the reference program's by a relative error of at most 0.0015.
Values may be sent and summed in bfloat16 or wider, within the bound.
A program may use at most 64 MiB of HBM per device.

```python
import jax
import jax.numpy as jnp
from jax import lax

BLOCK = 256
ROW_BLK = 16
COL_BLK = 48
SLOTS = 2
ITERS = 8
ROW_BLOCKS = 256
ROWS = 65536
COLS = 196608
N_ROW = 16
N_COL = 16


def draw_block_cols(key, part):
    row_total = ROW_BLK * N_ROW
    group_total = N_COL
    key_perm = jax.random.fold_in(key, 11)
    key_live = jax.random.fold_in(key, 23)
    key_place = jax.random.fold_in(key, 37)
    perm_keys = jax.random.split(key_perm, row_total * group_total)
    picked_cols = jax.vmap(lambda single: jax.random.permutation(single, COL_BLK)[:SLOTS])(perm_keys)
    picked_cols = picked_cols.reshape(row_total, group_total, SLOTS).astype(jnp.int32)
    live_count = jax.random.randint(key_live, (row_total, group_total), 0, SLOTS + 1)
    place_row = jax.random.randint(key_place, (), 0, row_total)
    place_group = jax.random.randint(jax.random.fold_in(key_place, 5), (), 0, group_total)
    forced = (jnp.arange(row_total, dtype=jnp.int32)[:, None] == place_row) & (jnp.arange(group_total, dtype=jnp.int32)[None, :] == place_group)
    live_count = jnp.where(forced, SLOTS, live_count)
    slot_index = jnp.arange(SLOTS, dtype=jnp.int32)[None, None, :]
    result = jnp.where(slot_index < live_count[:, :, None], picked_cols, COL_BLK)
    return result.reshape(row_total, group_total * SLOTS).astype(jnp.int32)


def block_levels(key, shape, pieces, low, top_value):
    level = 1.0
    for dim, blocks in pieces:
        steps = jax.random.uniform(jax.random.fold_in(jax.random.fold_in(key, 6), dim), (blocks,), jnp.float32, low / len(pieces), top_value / len(pieces))
        level = level * jnp.repeat(jnp.exp(steps), shape[dim] // blocks).reshape((-1,) + (1,) * (len(shape) - 1 - dim))
    return level


def centred(stream_key, shape, deviation, most, cuts=(), kind=jnp.bfloat16):
    loudness = block_levels(stream_key, shape, cuts, -0.22, 0.18) if cuts else 1.0
    values = jax.random.normal(stream_key, shape, jnp.float32) * deviation * loudness
    return jnp.minimum(jnp.maximum(values, -most), most).astype(kind)


def setup_inputs(seed: int = 0) -> dict:
    arg_keys = jax.random.split(jax.random.key(seed), 9)
    return {
        "blocks": centred(arg_keys[0], (ROW_BLOCKS, N_COL * SLOTS, BLOCK, BLOCK), (BLOCK * SLOTS * N_COL) ** -0.5, 0.0625, ((0, 16), (1, 16))),
        "block_cols": draw_block_cols(jax.random.fold_in(arg_keys[8], 71), 0),
        "objective": centred(arg_keys[2], (COLS,), 1.0, 6.0, ((0, 256),), jnp.float32),
        "lower_bound": jnp.clip(-1.0 + 0.8 * jax.random.uniform(arg_keys[3], (COLS,), jnp.float32) ** block_levels(arg_keys[3], (COLS,), ((0, 256),), -0.2, 0.2), -1.0, -0.2),
        "upper_bound": jnp.clip(0.2 + 0.8 * jax.random.uniform(arg_keys[4], (COLS,), jnp.float32) ** block_levels(arg_keys[4], (COLS,), ((0, 256),), -0.2, 0.2), 0.2, 1.0),
        "right_side": centred(arg_keys[5], (ROWS,), 1.0, 6.0, ((0, 256),), jnp.float32),
        "primal_init": jnp.clip(jax.random.uniform(arg_keys[6], (COLS,), jnp.float32, -0.2, 0.2) * block_levels(arg_keys[6], (COLS,), ((0, 256),), -0.4, 0.0), -0.2, 0.2),
        "dual_init": jnp.clip(1.0 * jax.random.uniform(arg_keys[7], (ROWS,), jnp.float32) ** block_levels(arg_keys[7], (ROWS,), ((0, 256),), -0.2, 0.2), 0.0, 1.0),
    }


step_primal = 0.5
step_dual = 0.5

def reference(blocks, block_cols, objective, lower_bound, upper_bound, right_side, primal_init, dual_init):
    total_blocks = blocks.shape[0]
    slot_total = blocks.shape[1]
    width = blocks.shape[2]
    col_total = COL_BLK * N_COL
    live = block_cols < COL_BLK
    group = jnp.arange(slot_total, dtype=jnp.int32) // SLOTS
    indices = jnp.where(live, group[None, :] * COL_BLK + block_cols, 0).astype(jnp.int32)
    weight_mask = live.astype(jnp.float32)
    grouped_blocks = blocks.reshape(N_ROW, total_blocks // N_ROW, slot_total, width, width)
    grouped_idx = indices.reshape(N_ROW, total_blocks // N_ROW, slot_total)
    grouped_mask = weight_mask.reshape(N_ROW, total_blocks // N_ROW, slot_total)

    def times_matrix(vector_half):
        lookup = vector_half.astype(jnp.float32).reshape(col_total, width)

        def one_group(packed):
            block_group, index_group, mask_group = packed
            picked = lookup[index_group] * mask_group[:, :, None]
            return jnp.einsum('gjab,gjb->ga', block_group.astype(jnp.float32), picked, precision=lax.Precision.HIGHEST)
        return lax.map(one_group, (grouped_blocks, grouped_idx, grouped_mask)).reshape(-1)

    def times_transpose(vector_half):
        values = vector_half.astype(jnp.float32).reshape(N_ROW, total_blocks // N_ROW, width)

        def one_group(packed):
            block_group, value_group, mask_group = packed
            contrib = jnp.einsum('gjab,ga->gjb', block_group.astype(jnp.float32), value_group, precision=lax.Precision.HIGHEST)
            return contrib * mask_group[:, :, None]
        contrib = lax.map(one_group, (grouped_blocks, values, grouped_mask))
        summed = jax.ops.segment_sum(contrib.reshape(-1, width), indices.reshape(-1), num_segments=col_total)
        return summed.reshape(-1)
    primal_now = primal_init
    dual_now = dual_init
    history = []
    for iteration in range(ITERS):
        dual_half = dual_now.astype(jnp.bfloat16)
        gradient = times_transpose(dual_half)
        primal_next = jnp.minimum(upper_bound, jnp.maximum(lower_bound, primal_now - step_primal * (objective - gradient)))
        extrapolated = (2.0 * primal_next - primal_now).astype(jnp.bfloat16)
        image_dual = times_matrix(extrapolated)
        dual_next = jnp.maximum(dual_now + step_dual * (right_side - image_dual), 0.0)
        primal_step = primal_next - primal_now
        dual_step = dual_next - dual_now
        history.append(jnp.stack((jnp.sqrt(jnp.mean(primal_step * primal_step)), jnp.sqrt(jnp.mean(dual_step * dual_step)))))
        primal_now = primal_next
        dual_now = dual_next
    return (primal_now, dual_now, jnp.stack(history))
```

```python
import functools

import jax
import jax.numpy as jnp
from jax import lax
from jax.experimental import pallas as pl
from jax.experimental.pallas import tpu as pltpu
from jax.sharding import PartitionSpec as P

MESH = pl.DeviceIdType.MESH
ITERS = 8
W = 256
H = 128
NX = 4
STEP = 0.5
CHUNKS = 4
F32 = jnp.float32
BF16 = jnp.bfloat16


def hops(d, n):
    return min(d, n - d)


def ring_order(n):
    return sorted(range(1, n), key=lambda d: -hops(d, n))


def plane_order(ny, nx):
    pairs = [(dy, dx) for dy in range(ny) for dx in range(nx) if (dy, dx) != (0, 0)]
    return sorted(pairs, key=lambda p: -(hops(p[0], ny) + hops(p[1], nx)))


def kernel(
    nz, ny, nx,
    cols, blocks, objective, lower, upper, right_side, primal_init, dual_init,
    primal_out, dual_out, norms_out,
    bl, bt, mask, left, left2, slab, dslab, yf,
    pinit, pgot, dinit, dgot,
    gsend, grecv, zsend, zrecv, esend, erecv, xg, gath, xsend, xrecv,
    pacc, dacc, prow, precv, frow, frecv, plast, pstage, dstage,
    sem_blk, sem_in, sem_out,
    s_pinit, r_pinit, s_dinit, r_dinit,
    s_g, r_g, s_e, r_e, s_z, r_z, s_x, r_x,
    s_p, r_p, s_f, r_f, s_l, r_l,
):
    nrow, ncol = nz * 2, ny * nx
    rb, cb = ncol, 3 * nrow
    kg = rb * 2 * W
    row = lax.axis_index("row")
    col = lax.axis_index("col")
    z, c = row // 2, row % 2
    y, x = col // nx, col % nx
    other = 1 - c
    partner = (z * 2 + other, col)

    zpeers = [lax.rem(z + d, nz) for d in ring_order(nz)]
    xpeers = [lax.rem(y + dy, ny) * nx + lax.rem(x + dx, nx) for dy, dx in plane_order(ny, nx)]

    def remote(src, dst, ssem, rsem, dev):
        return pltpu.make_async_remote_copy(
            src_ref=src, dst_ref=dst, send_sem=ssem, recv_sem=rsem,
            device_id=dev, device_id_type=MESH,
        )

    rows_per = kg // CHUNKS
    for j in range(CHUNKS):
        pltpu.make_async_copy(
            blocks.at[pl.ds(j * rows_per, rows_per)], bl.at[pl.ds(j * rows_per, rows_per)], sem_blk.at[j]
        ).start()
    loads = []
    for q, ref in enumerate((dual_init, right_side)):
        for h in range(2):
            loads.append(pltpu.make_async_copy(ref.at[pl.ds(h * H, H)], dinit.at[q * 2 + h, 0], sem_in.at[len(loads)]))
    nd = len(loads)
    for q, ref in enumerate((primal_init, objective, lower, upper)):
        for i in range(3):
            for h in range(2):
                loads.append(
                    pltpu.make_async_copy(
                        ref.at[pl.ds(i * W + h * H, H)], pinit.at[h * 12 + q * 3 + i, 0], sem_in.at[len(loads)]
                    )
                )
    for cp in loads:
        cp.start()

    barrier = pltpu.get_barrier_semaphore()
    group = [partner]
    for zp in zpeers:
        group += [(zp * 2, col), (zp * 2 + 1, col)]
    xgroup = [(row, xp) for xp in xpeers]
    for dev in xgroup + group:
        pl.semaphore_signal(barrier, inc=1, device_id=dev, device_id_type=MESH)
    for cp in loads:
        cp.wait()
    pl.semaphore_wait(barrier, len(group) + len(xgroup))

    for i, dev in enumerate(xgroup):
        remote(dinit, dgot.at[pl.ds(col * 4, 4)], s_dinit.at[i], r_dinit.at[col], dev).start()
    pdest = [(partner, other)]
    for zp in zpeers:
        pdest += [((zp * 2 + h, col), h) for h in (0, 1)]
    for i, (dev, h) in enumerate(pdest):
        remote(pinit.at[pl.ds(h * 12, 12)], pgot.at[pl.ds(row * 12, 12)], s_pinit.at[i], r_pinit.at[row], dev).start()
    dgot[pl.ds(col * 4, 4)] = dinit[...]
    pgot[pl.ds(row * 12, 12)] = pinit[pl.ds(c * 12, 12)]

    slot_id = lax.broadcasted_iota(jnp.int32, (cb, H), 0)
    for r in range(rb):
        for s in range(2):
            mask[r * 2 + s] = jnp.where(slot_id == cols[r, s], 1.0, 0.0).astype(BF16)
    xg[...] = jnp.zeros_like(xg)
    pacc[...] = jnp.zeros_like(pacc)
    dacc[...] = jnp.zeros_like(dacc)
    eye = jnp.where(
        lax.broadcasted_iota(jnp.int32, (W, W), 0) == lax.broadcasted_iota(jnp.int32, (W, W), 1), 1.0, 0.0
    ).astype(BF16)
    for j in range(CHUNKS):
        pltpu.make_async_copy(
            blocks.at[pl.ds(j * rows_per, rows_per)], bl.at[pl.ds(j * rows_per, rows_per)], sem_blk.at[j]
        ).wait()

    def turn(rs, carry):
        block = bl[pl.ds(pl.multiple_of(rs * W, W), W), :]
        turned = lax.dot_general(eye, block, (((1,), (1,)), ((), ())), preferred_element_type=F32).astype(BF16)
        at = pl.ds(pl.multiple_of(rs * H, H), H)
        bt[0, at, :] = turned[:H]
        bt[1, at, :] = turned[H:]
        return carry

    lax.fori_loop(0, rb * 2, turn, 0)

    for i, dev in enumerate(xgroup):
        src = xpeers[i]
        remote(dinit, dgot.at[pl.ds(src * 4, 4)], s_dinit.at[i], r_dinit.at[src], dev).wait_recv()
    for g in range(ncol):
        for q in range(2):
            for h in range(2):
                dslab[q, g : g + 1, h * H : (h + 1) * H] = dgot[g * 4 + q * 2 + h]

    lane8 = lax.broadcasted_iota(jnp.int32, (8, H), 1)
    sub8 = lax.broadcasted_iota(jnp.int32, (8, H), 0)

    def to_lanes(acc, off):
        total = jnp.sum(acc, axis=1, keepdims=True)
        return jnp.sum(jnp.where(lane8 == sub8 + off, total, 0.0), axis=0, keepdims=True)

    row_id = lax.broadcasted_iota(jnp.int32, (rb, H), 0)

    def half_gradient(h):
        acc = jnp.zeros((cb, H), F32)
        lanes = pl.ds(pl.multiple_of(h * H, H), H)
        step = kg // CHUNKS
        for j in range(CHUNKS):
            acc = acc + jnp.dot(
                left[:, j * step : (j + 1) * step], bl[j * step : (j + 1) * step, lanes], preferred_element_type=F32
            )
        return acc

    def half_image(which, h):
        for r in range(rb):
            for s in range(2):
                gath[s, r : r + 1, :] = xg[which, pl.ds(cols[r, s], 1), :]
        picked = [gath[s].astype(BF16) for s in range(2)]
        for r in range(rb):
            keep = jnp.where(row_id == r, 1.0, 0.0).astype(BF16)
            for s in range(2):
                left2[:, (r * 2 + s) * H : (r * 2 + s + 1) * H] = picked[s] * keep
        acc = jnp.zeros((rb, W), F32)
        step = rb * W // CHUNKS
        for j in range(CHUNKS):
            acc = acc + jnp.dot(
                left2[:, j * step : (j + 1) * step], bt[h, j * step : (j + 1) * step, :], preferred_element_type=F32
            )
        return acc

    def iteration(k, carry):
        par = lax.rem(k, 2)
        yf[...] = dslab[0].astype(BF16).astype(F32)
        for r in range(rb):
            wide = jnp.broadcast_to(yf[r : r + 1, :], (cb, W)).astype(BF16)
            for s in range(2):
                m = mask[r * 2 + s]
                for h in range(2):
                    at = (r * 2 + s) * W + h * H
                    left[:, at : at + H] = wide[:, h * H : (h + 1) * H] * m
        gsend[...] = half_gradient(other)
        to_partner = remote(gsend, grecv, s_g, r_g, partner)
        to_partner.start()
        own = half_gradient(c)
        to_partner.wait()
        total = (own + grecv[...]).astype(BF16)
        zsend[par] = total
        zrecv[par, z] = total
        sends = [
            remote(zsend.at[par], zrecv.at[par, z], s_z.at[i], r_z.at[par, z], (zp * 2 + c, col))
            for i, zp in enumerate(zpeers)
        ]
        for cp in sends:
            cp.start()

        @pl.when(k == 0)
        def _():
            for i, (dev, h) in enumerate(pdest):
                src = dev[0]
                remote(
                    pinit.at[pl.ds(h * 12, 12)], pgot.at[pl.ds(src * 12, 12)], s_pinit.at[i], r_pinit.at[src], dev
                ).wait_recv()
            for q in range(4):
                for i in range(nrow):
                    for b in range(3):
                        slab[q, i * 3 + b : i * 3 + b + 1, :] = pgot[i * 12 + q * 3 + b]

        for i, zp in enumerate(zpeers):
            remote(zsend.at[par], zrecv.at[par, zp], s_z.at[i], r_z.at[par, zp], (zp * 2 + c, col)).wait_recv()
        grad = zrecv[par, 0].astype(F32)
        for i in range(1, nz):
            grad = grad + zrecv[par, i].astype(F32)
        now = slab[0]
        new = jnp.minimum(slab[3], jnp.maximum(slab[2], now - STEP * (slab[1] - grad)))
        ext = (2.0 * new - now).astype(BF16)
        esend[...] = ext
        xg[0, 0:cb, :] = ext.astype(F32)
        to_partner2 = remote(esend, erecv, s_e, r_e, partner)
        to_partner2.start()
        slab[0] = new
        pstep = new - now
        pacc[pl.ds(k, 1), :] = jnp.sum(pstep * pstep, axis=0, keepdims=True)
        image = half_image(0, c)
        to_partner2.wait()
        xg[1, 0:cb, :] = erecv[...].astype(F32)
        image = (image + half_image(1, other)).astype(BF16)
        xsend[par] = image
        xrecv[par, col] = image
        for i, xp in enumerate(xpeers):
            remote(xsend.at[par], xrecv.at[par, col], s_x.at[i], r_x.at[par, col], (row, xp)).start()

        @pl.when(k == ITERS - 1)
        def _():
            prow[0] = to_lanes(pacc[...], 8)
            precv[col] = prow[0]
            plast[0] = slab[0]
            for i, xp in enumerate(xpeers):
                remote(prow, precv.at[pl.ds(col, 1)], s_p.at[i], r_p.at[col], (row, xp)).start()
            remote(plast.at[0], plast.at[1], s_l, r_l, partner).start()

        for i, zp in enumerate(zpeers):
            sends[i].wait_send()
        for i, xp in enumerate(xpeers):
            remote(xsend.at[par], xrecv.at[par, xp], s_x.at[i], r_x.at[par, xp], (row, xp)).wait()
        img = xrecv[par, 0].astype(F32)
        for i in range(1, ncol):
            img = img + xrecv[par, i].astype(F32)
        dnow = dslab[0]
        dnew = jnp.maximum(dnow + STEP * (dslab[1] - img), 0.0)
        dslab[0] = dnew
        dstep = dnew - dnow
        drow = jnp.sum(dstep * dstep, axis=0, keepdims=True)
        dacc[pl.ds(k, 1), :] = drow[:, :H] + drow[:, H:]
        return carry

    lax.fori_loop(0, ITERS, iteration, 0)

    for i, xp in enumerate(xpeers):
        remote(prow, precv.at[pl.ds(xp, 1)], s_p.at[i], r_p.at[xp], (row, xp)).wait()
    ptotal = precv[0]
    for i in range(1, ncol):
        ptotal = ptotal + precv[i]
    mine = to_lanes(dacc[...], 0) + ptotal
    frow[0] = mine
    frecv[row] = mine
    for i, dev in enumerate(group):
        remote(frow, frecv.at[pl.ds(row, 1)], s_f.at[i], r_f.at[row], dev).start()

    remote(plast.at[0], plast.at[1], s_l, r_l, partner).wait()
    for b in range(3):
        at = row * 3 + b
        pstage[pl.ds(b * 2 + c, 1), 0] = plast[0, pl.ds(at, 1), :]
        pstage[pl.ds(b * 2 + other, 1), 0] = plast[1, pl.ds(at, 1), :]
    for h in range(2):
        gath[h] = dslab[0, :, h * H : (h + 1) * H]
        dstage[h] = gath[h, pl.ds(col, 1), :]
    outs = [pltpu.make_async_copy(pstage.at[i, 0], primal_out.at[pl.ds(i * H, H)], sem_out.at[i]) for i in range(6)]
    outs += [pltpu.make_async_copy(dstage.at[h, 0], dual_out.at[pl.ds(h * H, H)], sem_out.at[6 + h]) for h in range(2)]
    for cp in outs:
        cp.start()
    for i in range(len(xgroup)):
        remote(dinit, dgot.at[pl.ds(0, 4)], s_dinit.at[i], r_dinit.at[0], xgroup[i]).wait_send()
    for i, (dev, h) in enumerate(pdest):
        remote(pinit.at[pl.ds(h * 12, 12)], pgot.at[pl.ds(0, 12)], s_pinit.at[i], r_pinit.at[0], dev).wait_send()
    for cp in outs:
        cp.wait()
    for i, dev in enumerate(group):
        remote(frow, frecv.at[pl.ds(dev[0], 1)], s_f.at[i], r_f.at[dev[0]], dev).wait()
    dsum = frecv[0]
    for i in range(1, nrow):
        dsum = dsum + frecv[i]
    psum = frecv[z * 2] + frecv[z * 2 + 1]
    dcol = jnp.sum(jnp.where(lane8 == sub8, dsum, 0.0), axis=1, keepdims=True)
    pcol = jnp.sum(jnp.where(lane8 == sub8 + 8, psum, 0.0), axis=1, keepdims=True)
    ptot = float(cb * W * ncol)
    dtot = float(rb * W * nrow)
    pair = lax.broadcasted_iota(jnp.int32, (8, 2), 1)
    norms_out[...] = jnp.sqrt(jnp.where(pair == 0, pcol * (1.0 / ptot), dcol * (1.0 / dtot)))


def per_device(nz, ny, nx, blocks, block_cols, objective, lower_bound, upper_bound, right_side, primal_init, dual_init):
    nrow, ncol = nz * 2, ny * nx
    rb, cb = ncol, 3 * nrow
    kg = rb * 2 * W
    hbm = pl.BlockSpec(memory_space=pl.ANY)
    V, D = pltpu.VMEM, pltpu.SemaphoreType.DMA
    nzp, nxp, ngr = nz - 1, ncol - 1, 2 * nz - 1
    return pl.pallas_call(
        functools.partial(kernel, nz, ny, nx),
        out_shape=(
            jax.ShapeDtypeStruct((3 * W,), F32),
            jax.ShapeDtypeStruct((W,), F32),
            jax.ShapeDtypeStruct((ITERS, 2), F32),
        ),
        in_specs=[pl.BlockSpec(memory_space=pltpu.SMEM)] + [hbm] * 7,
        out_specs=(hbm, hbm, pl.BlockSpec(memory_space=pltpu.VMEM)),
        scratch_shapes=[
            V((kg, W), BF16),
            V((2, rb * W, W), BF16),
            V((rb * 2, cb, H), BF16),
            V((cb, kg), BF16),
            V((rb, rb * W), BF16),
            V((4, cb, H), F32),
            V((2, rb, W), F32),
            V((rb, W), F32),
            V((24, 1, H), F32),
            V((nrow * 12, 1, H), F32),
            V((4, 1, H), F32),
            V((ncol * 4, 1, H), F32),
            V((cb, H), F32),
            V((cb, H), F32),
            V((2, cb, H), BF16),
            V((2, nz, cb, H), BF16),
            V((cb, H), BF16),
            V((cb, H), BF16),
            V((2, cb + 8, H), F32),
            V((2, rb, H), F32),
            V((2, rb, W), BF16),
            V((2, ncol, rb, W), BF16),
            V((8, H), F32),
            V((8, H), F32),
            V((1, 1, H), F32),
            V((ncol, 1, H), F32),
            V((1, 1, H), F32),
            V((nrow, 1, H), F32),
            V((2, cb, H), F32),
            V((6, 1, H), F32),
            V((2, 1, H), F32),
            D((CHUNKS,)),
            D((28,)),
            D((8,)),
            D((ngr,)), D((nrow,)), D((nxp,)), D((ncol,)),
            D(()), D(()), D(()), D(()),
            D((nzp,)), D((2, nz)), D((nxp,)), D((2, ncol)),
            D((nxp,)), D((ncol,)), D((ngr,)), D((nrow,)),
            D(()), D(()),
        ],
        compiler_params=pltpu.CompilerParams(
            collective_id=0, has_side_effects=True, vmem_limit_bytes=48 * 1024 * 1024
        ),
    )(
        block_cols, blocks.reshape(kg, W), objective, lower_bound, upper_bound, right_side, primal_init, dual_init
    )


def solution(mesh):
    nz = mesh.shape["row"] // 2
    nx = NX if mesh.shape["col"] == NX * NX else 2
    ny = mesh.shape["col"] // nx
    placed = (
        P("row", "col", None, None),
        P("row", "col"),
        P(("col", "row")),
        P(("col", "row")),
        P(("col", "row")),
        P(("row", "col")),
        P(("col", "row")),
        P(("row", "col")),
    )
    return jax.shard_map(
        functools.partial(per_device, nz, ny, nx),
        mesh=mesh,
        in_specs=placed,
        out_specs=(P(("col", "row")), P(("row", "col")), P()),
        check_vma=False,
    )
```
